32 devices in a mesh: gx: 4 (over z), gy: 8 (over y, x, core).
Axes of the slice: x: 2, y: 2, z: 4, core: 2. Of those that a mesh axis runs over, the one named last changes fastest.
Arguments:
- tables: float32 [2, 262144, 128], P(None, ('gx', 'gy')), may hold values from -0.9 to 0.9
- cold_rows: int32 [32, 2, 32, 16], P(('gx', 'gy')), may hold values from 0 to 8191, as said below
- cold_bags: int32 [32, 2, 32, 16], P(('gx', 'gy')), may hold values from -1 to 127, as said below
- hot_rows: int32 [2, 256], replicated, may hold values from 0 to 262143
- hot_ids: int32 [4096, 2, 8], P(('gx', 'gy')), may hold values from 0 to 255
Outputs:
- pooled: float32 [4096, 2, 128], P(('gx', 'gy'))
The draws below stay inside these ranges and needn't reach their ends.
Inputs may be any that keep to these rules, and one draw needn't show every extreme that they name: `cold_rows`: every entry names one of the owner's 8192 rows. `cold_bags`: live slots of one sender, table and owner come first, the empty ones (-1) after them; in every draw each table has an owner whose 16 slots are all live from every sender.
All inputs are finite; a program needn't handle non-finite values.
Results may differ from the reference program's by a relative error of at most 0.0003.
Values sent between devices are 32-bit elements; how exact they have to be, the bound alone decides.
No kernel may reach another device: no remote copies, remote signals or barrier semaphores. Data moves between devices by JAX's collectives and lax.ppermute only.
A program may use at most 64 MiB of HBM per device.

```python
import jax
import jax.numpy as jnp
from jax import lax

DIM = 128
ROWS_DEV = 8192
TABLES = 2
BATCH_DEV = 128
CAP = 16
HOT = 256
HOT_BAG = 8
PEERS = 32
BATCH = 4096
ROWS = 262144


def draw_cold_rows(key, part):
    shape_all = (PEERS, TABLES, PEERS, CAP)
    exponent = jax.random.randint(jax.random.fold_in(key, 101), shape_all, 0, 21)
    limit = jnp.minimum(jnp.left_shift(jnp.ones(shape_all, jnp.int32), exponent), ROWS_DEV)
    return jax.random.randint(jax.random.fold_in(key, 102), shape_all, 0, limit).astype(jnp.int32)


def draw_cold_bags(key, part):
    shape_all = (PEERS, TABLES, PEERS, CAP)
    busiest = jax.random.randint(jax.random.fold_in(key, 201), (TABLES,), 0, PEERS)
    filled = jax.random.randint(jax.random.fold_in(key, 202), (PEERS, TABLES, PEERS), max(1, CAP // 4), CAP + 1)
    owner_index = jnp.arange(PEERS, dtype=jnp.int32)[None, None, :]
    filled = jnp.where(owner_index == busiest[None, :, None], CAP, filled)
    samples = jax.random.randint(jax.random.fold_in(key, 203), shape_all, 0, BATCH_DEV)
    slot_index = jnp.arange(CAP, dtype=jnp.int32)
    return jnp.where(slot_index < filled[..., None], samples, -1).astype(jnp.int32)


def place_ends(entries, rng, smallest, largest):
    longest = entries.shape.index(max(entries.shape))
    spots = []
    for shift in (0, 1):
        where = [jax.random.randint(jax.random.fold_in(rng, axis), (), 0, length) for axis, length in enumerate(entries.shape)]
        where[longest] = (where[longest] + shift) % entries.shape[longest]
        spots.append(tuple(where))
    return entries.at[spots[0]].set(smallest).at[spots[1]].set(largest)


def shard_levels(own_key, extent, pieces, least, high):
    def one(position, parts):
        draws = jax.random.uniform(jax.random.fold_in(jax.random.fold_in(own_key, 6), position), (parts,), jnp.float32, least / len(pieces), high / len(pieces))
        return jnp.repeat(jnp.exp(draws), extent[position] // parts).reshape((-1,) + (1,) * (len(extent) - position - 1))

    gain = one(*pieces[0])
    for cut in pieces[1:]:
        gain = gain * one(*cut)
    return gain


def centred(stream_key, shape, deviation, reach, cuts=(), kind=jnp.bfloat16):
    drawn = jax.random.normal(stream_key, shape, jnp.float32) * deviation
    if len(cuts) > 0:
        drawn = shard_levels(stream_key, shape, cuts, -0.22, 0.18) * drawn
    return jnp.clip(drawn, min=-reach, max=reach).astype(kind)


def setup_inputs(seed: int = 0) -> dict:
    key_list = jax.random.split(jax.random.key(seed), 6)
    return {
        "tables": centred(key_list[0], (TABLES, ROWS, DIM), 0.15, 0.9, ((1, 32),), jnp.float32),
        "cold_rows": draw_cold_rows(jax.random.fold_in(key_list[5], 71), 0),
        "cold_bags": draw_cold_bags(jax.random.fold_in(key_list[5], 71), 0),
        "hot_rows": place_ends(jax.random.randint(key_list[3], (TABLES, HOT), 0, ROWS), jax.random.fold_in(key_list[3], 1), 0, ROWS - 1).astype(jnp.int32),
        "hot_ids": place_ends(jax.random.randint(key_list[4], (BATCH, TABLES, HOT_BAG), 0, HOT), jax.random.fold_in(key_list[4], 1), 0, HOT - 1).astype(jnp.int32),
    }


def take_rows(matrix, indices):
    return jnp.take(matrix, indices, axis=0)


def reference(tables, cold_rows, cold_bags, hot_rows, hot_ids):
    offsets = (jnp.arange(PEERS, dtype=jnp.int32) * ROWS_DEV)[:, None]

    def per_table(table_index):
        one_table = tables[table_index]

        def per_sender(sender):
            slot_rows = (cold_rows[sender, table_index] + offsets).reshape(-1)
            slot_bags = cold_bags[sender, table_index].reshape(-1)
            looked = take_rows(one_table, slot_rows)
            live_mask = slot_bags >= 0
            segment = jnp.where(live_mask, slot_bags, 0).astype(jnp.int32)
            values = jnp.where(live_mask[:, None], looked, jnp.zeros_like(looked))
            return jax.ops.segment_sum(values, segment, num_segments=BATCH_DEV)

        return lax.map(per_sender, jnp.arange(PEERS, dtype=jnp.int32))

    cold_part = lax.map(per_table, jnp.arange(TABLES, dtype=jnp.int32))
    cold_part = jnp.transpose(cold_part, (1, 2, 0, 3)).reshape(BATCH, TABLES, DIM)
    hot_table = jax.vmap(take_rows)(tables, hot_rows)

    def pool_hot(table_rows, lookups):
        return jnp.sum(take_rows(table_rows, lookups), axis=1)

    hot_part = jax.vmap(pool_hot, in_axes=(0, 1), out_axes=1)(hot_table, hot_ids)
    return cold_part + hot_part
```

```python
import jax
import jax.numpy as jnp
from jax import lax
from jax.experimental import pallas as pl
from jax.experimental.pallas import tpu as pltpu
from jax.sharding import PartitionSpec as P


AXES = ("gx", "gy")


def push_hot(peers, tables, hot_each, rows_dev, base_ref, hot_ref, index_ref, table_ref, out_ref, sem):
    chunk = tables * hot_each + 1
    out_ref[...] = jnp.zeros_like(out_ref)
    base = base_ref[0]

    def one_peer(peer, count):
        for t in range(tables):
            for s in range(hot_each):
                row = hot_ref[t, peer * hot_each + s] - base
                mine = jnp.logical_and(row >= 0, row < rows_dev)

                @pl.when(mine)
                def _():
                    pltpu.make_async_copy(
                        table_ref.at[t * rows_dev + row],
                        out_ref.at[peer * chunk + t * hot_each + s],
                        sem,
                    ).start()

                count = count + mine.astype(jnp.int32)
        out_ref[peer * chunk + chunk - 1] = index_ref[peer]
        return count

    count = lax.fori_loop(0, peers, one_peer, jnp.int32(0))

    @pl.when(count > 0)
    def _():
        pltpu.make_async_copy(
            table_ref.at[pl.ds(0, count)], out_ref.at[pl.ds(0, count)], sem
        ).wait()


def look_up(peers, tables, slots, hot_each, rows_dev, rows_ref, hot_ref, table_ref, out_ref, sem):
    cold = tables * slots
    hot = tables * hot_each
    chunk = cold + hot

    def one_peer(peer, carry):
        for t in range(tables):
            for c in range(slots):
                row = rows_ref[peer, t * slots + c]
                pltpu.make_async_copy(
                    table_ref.at[t * rows_dev + row],
                    out_ref.at[peer * chunk + t * slots + c],
                    sem,
                ).start()
        return carry

    lax.fori_loop(0, peers, one_peer, 0)
    total = hot_ref[0, pl.ds(0, hot)]
    for peer in range(1, peers):
        total = total + hot_ref[peer, pl.ds(0, hot)]
    for peer in range(peers):
        out_ref[pl.ds(peer * chunk + cold, hot)] = total
    pltpu.make_async_copy(
        table_ref.at[pl.ds(0, peers * cold)], out_ref.at[pl.ds(0, peers * cold)], sem
    ).wait()


def pool(tables, bags_ref, names_ref, ids_ref, rows_ref, out_ref):
    batch = out_ref.shape[0]
    count = rows_ref.shape[0]
    sample = lax.broadcasted_iota(jnp.int32, (batch, count), 0)
    picks = []
    for t in range(tables):
        hits = (bags_ref[pl.ds(t, 1), :] == sample).astype(jnp.float32)
        names = names_ref[pl.ds(t, 1), :]
        for k in range(ids_ref.shape[2]):
            hits = hits + (ids_ref[t, :, k : k + 1] == names).astype(jnp.float32)
        picks.append(hits.astype(jnp.bfloat16))
    rows = rows_ref[...]
    high = rows.astype(jnp.bfloat16)
    rest = rows - high.astype(jnp.float32)
    mid = rest.astype(jnp.bfloat16)
    low = (rest - mid.astype(jnp.float32)).astype(jnp.bfloat16)
    for t in range(tables):
        part = jnp.dot(picks[t], low, preferred_element_type=jnp.float32)
        part = part + jnp.dot(picks[t], mid, preferred_element_type=jnp.float32)
        part = part + jnp.dot(picks[t], high, preferred_element_type=jnp.float32)
        out_ref[:, t, :] = part


def body(tables, cold_rows, cold_bags, hot_rows, hot_ids):
    peers = lax.axis_size("gx") * lax.axis_size("gy")
    table_count, rows_dev, width = tables.shape
    slots = cold_rows.shape[3]
    batch = hot_ids.shape[0]
    hot_count = hot_rows.shape[1]
    hot_each = -(-hot_count // peers)
    cold = table_count * slots
    hot = table_count * hot_each
    base = (lax.axis_index(AXES) * rows_dev).astype(jnp.int32).reshape(1)
    hot_rows = jnp.pad(hot_rows, ((0, 0), (0, hot_each * peers - hot_count)), constant_values=-1)
    flat = tables.reshape(table_count * rows_dev, 1, width)
    lanes = -(-cold // width)
    assert lanes == 1
    wanted = jnp.transpose(cold_rows[0], (1, 0, 2)).reshape(peers, 1, cold).astype(jnp.float32)
    wanted = jnp.pad(wanted, ((0, 0), (0, 0), (0, width - cold)))

    smem = pl.BlockSpec(memory_space=pltpu.SMEM)
    vmem = pl.BlockSpec(memory_space=pltpu.VMEM)
    anywhere = pl.BlockSpec(memory_space=pl.ANY)

    first = pl.pallas_call(
        lambda *refs: push_hot(peers, table_count, hot_each, rows_dev, *refs),
        out_shape=jax.ShapeDtypeStruct((peers * (hot + 1), 1, width), jnp.float32),
        in_specs=[smem, smem, vmem, anywhere],
        out_specs=vmem,
        scratch_shapes=[pltpu.SemaphoreType.DMA],
        name="push_hot",
    )(base, hot_rows, wanted, flat)
    first = first.reshape(peers, hot + 1, 1, width)
    first = lax.all_to_all(first, AXES, split_axis=0, concat_axis=0, tiled=True)
    asked = first[:, hot, 0, :cold].astype(jnp.int32)

    second = pl.pallas_call(
        lambda *refs: look_up(peers, table_count, slots, hot_each, rows_dev, *refs),
        out_shape=jax.ShapeDtypeStruct((peers * (cold + hot), 1, width), jnp.float32),
        in_specs=[smem, vmem, anywhere],
        out_specs=vmem,
        scratch_shapes=[pltpu.SemaphoreType.DMA],
        name="look_up",
    )(asked, first, flat)
    second = second.reshape(peers, cold + hot, 1, width)
    second = lax.all_to_all(second, AXES, split_axis=0, concat_axis=0, tiled=True)
    second = second.reshape(peers * (cold + hot), width)

    slot_table = jnp.arange(cold + hot, dtype=jnp.int32)
    bags = []
    names = []
    for t in range(table_count):
        bags.append(jnp.pad(cold_bags[0, t], ((0, 0), (t * slots, cold + hot - (t + 1) * slots)), constant_values=-1).reshape(-1))
        place = slot_table - cold - t * hot_each
        inside = jnp.logical_and(place >= 0, place < hot_each)
        peer = jnp.arange(peers, dtype=jnp.int32)[:, None]
        names.append(jnp.where(inside[None, :], peer * hot_each + place[None, :], -1).reshape(-1))
    return pl.pallas_call(
        lambda *refs: pool(table_count, *refs),
        out_shape=jax.ShapeDtypeStruct((batch, table_count, width), jnp.float32),
        in_specs=[vmem] * 4,
        out_specs=vmem,
        name="pool",
    )(jnp.stack(bags), jnp.stack(names), jnp.transpose(hot_ids, (1, 0, 2)), second)


def solution(mesh):
    return jax.shard_map(
        body,
        mesh=mesh,
        in_specs=(
            P(None, AXES, None),
            P(AXES, None, None, None),
            P(AXES, None, None, None),
            P(),
            P(AXES, None, None),
        ),
        out_specs=P(AXES, None, None),
        check_vma=False,
    )
```

```python
import jax
import jax.numpy as jnp
from jax import lax
from jax.experimental import pallas as pl
from jax.experimental.pallas import tpu as pltpu
from jax.sharding import PartitionSpec as P


AXES = ("gx", "gy")


def push_hot(peers, tables, hot_each, rows_dev, base_ref, hot_ref, index_ref, table_ref, out_ref, sem):
    chunk = tables * hot_each + 1
    out_ref[...] = jnp.zeros_like(out_ref)
    base = base_ref[0]

    def one_peer(peer, count):
        for t in range(tables):
            for s in range(hot_each):
                row = hot_ref[t, peer * hot_each + s] - base
                mine = jnp.logical_and(row >= 0, row < rows_dev)

                @pl.when(mine)
                def _():
                    pltpu.make_async_copy(
                        table_ref.at[t * rows_dev + row],
                        out_ref.at[peer * chunk + t * hot_each + s],
                        sem,
                    ).start()

                count = count + mine.astype(jnp.int32)
        out_ref[peer * chunk + chunk - 1] = index_ref[peer]
        return count

    count = lax.fori_loop(0, peers, one_peer, jnp.int32(0))

    @pl.when(count > 0)
    def _():
        pltpu.make_async_copy(
            table_ref.at[pl.ds(0, count)], out_ref.at[pl.ds(0, count)], sem
        ).wait()


def look_up(peers, tables, slots, hot_each, rows_dev, rows_ref, hot_ref, table_ref, out_ref, sem):
    cold = tables * slots
    hot = tables * hot_each
    chunk = cold + hot

    def one_peer(peer, carry):
        for t in range(tables):
            for c in range(slots):
                row = rows_ref[peer, t * slots + c]
                pltpu.make_async_copy(
                    table_ref.at[t * rows_dev + row],
                    out_ref.at[peer * chunk + t * slots + c],
                    sem,
                ).start()
        return carry

    lax.fori_loop(0, peers, one_peer, 0)
    total = hot_ref[0, pl.ds(0, hot)]
    for peer in range(1, peers):
        total = total + hot_ref[peer, pl.ds(0, hot)]
    for peer in range(peers):
        out_ref[pl.ds(peer * chunk + cold, hot)] = total
    pltpu.make_async_copy(
        table_ref.at[pl.ds(0, peers * cold)], out_ref.at[pl.ds(0, peers * cold)], sem
    ).wait()


def select(tables, bags_ref, names_ref, ids_ref, pick_ref):
    batch, count = pick_ref.shape[1:]
    sample = lax.broadcasted_iota(jnp.int32, (batch, count), 0)
    for t in range(tables):
        hits = (bags_ref[pl.ds(t, 1), :] == sample).astype(jnp.float32)
        names = names_ref[pl.ds(t, 1), :]
        for k in range(ids_ref.shape[2]):
            hits = hits + (ids_ref[t, :, k : k + 1] == names).astype(jnp.float32)
        pick_ref[t] = hits.astype(jnp.bfloat16)


def pool(tables, pick_ref, rows_ref, out_ref):
    rows = rows_ref[...]
    high = rows.astype(jnp.bfloat16)
    rest = rows - high.astype(jnp.float32)
    mid = rest.astype(jnp.bfloat16)
    low = (rest - mid.astype(jnp.float32)).astype(jnp.bfloat16)
    for t in range(tables):
        pick = pick_ref[t]
        part = jnp.dot(pick, low, preferred_element_type=jnp.float32)
        part = part + jnp.dot(pick, mid, preferred_element_type=jnp.float32)
        part = part + jnp.dot(pick, high, preferred_element_type=jnp.float32)
        out_ref[:, t, :] = part


def body(tables, cold_rows, cold_bags, hot_rows, hot_ids):
    peers = lax.axis_size("gx") * lax.axis_size("gy")
    table_count, rows_dev, width = tables.shape
    slots = cold_rows.shape[3]
    batch = hot_ids.shape[0]
    hot_count = hot_rows.shape[1]
    hot_each = -(-hot_count // peers)
    cold = table_count * slots
    hot = table_count * hot_each
    base = (lax.axis_index(AXES) * rows_dev).astype(jnp.int32).reshape(1)
    hot_rows = jnp.pad(hot_rows, ((0, 0), (0, hot_each * peers - hot_count)), constant_values=-1)
    flat = tables.reshape(table_count * rows_dev, 1, width)
    lanes = -(-cold // width)
    assert lanes == 1
    wanted = jnp.transpose(cold_rows[0], (1, 0, 2)).reshape(peers, 1, cold).astype(jnp.float32)
    wanted = jnp.pad(wanted, ((0, 0), (0, 0), (0, width - cold)))

    smem = pl.BlockSpec(memory_space=pltpu.SMEM)
    vmem = pl.BlockSpec(memory_space=pltpu.VMEM)
    anywhere = pl.BlockSpec(memory_space=pl.ANY)
    small = pltpu.CompilerParams(vmem_limit_bytes=24 * 1024 * 1024)

    first = pl.pallas_call(
        lambda *refs: push_hot(peers, table_count, hot_each, rows_dev, *refs),
        out_shape=jax.ShapeDtypeStruct((peers * (hot + 1), 1, width), jnp.float32),
        in_specs=[smem, smem, vmem, anywhere],
        out_specs=vmem,
        scratch_shapes=[pltpu.SemaphoreType.DMA],
        name="push_hot",
    )(base, hot_rows, wanted, flat)
    first = first.reshape(peers, hot + 1, 1, width)
    first = lax.all_to_all(first, AXES, split_axis=0, concat_axis=0, tiled=True)
    asked = first[:, hot, 0, :cold].astype(jnp.int32)

    second = pl.pallas_call(
        lambda *refs: look_up(peers, table_count, slots, hot_each, rows_dev, *refs),
        out_shape=jax.ShapeDtypeStruct((peers * (cold + hot), 1, width), jnp.float32),
        in_specs=[smem, vmem, anywhere],
        out_specs=vmem,
        scratch_shapes=[pltpu.SemaphoreType.DMA],
        name="look_up",
    )(asked, first, flat)
    second = second.reshape(peers, cold + hot, 1, width)
    second = lax.all_to_all(second, AXES, split_axis=0, concat_axis=0, tiled=True)
    second = second.reshape(peers * (cold + hot), width)

    slot_table = jnp.arange(cold + hot, dtype=jnp.int32)
    bags = []
    names = []
    for t in range(table_count):
        bags.append(jnp.pad(cold_bags[0, t], ((0, 0), (t * slots, cold + hot - (t + 1) * slots)), constant_values=-1).reshape(-1))
        place = slot_table - cold - t * hot_each
        inside = jnp.logical_and(place >= 0, place < hot_each)
        peer = jnp.arange(peers, dtype=jnp.int32)[:, None]
        names.append(jnp.where(inside[None, :], peer * hot_each + place[None, :], -1).reshape(-1))
    count = peers * (cold + hot)
    picks = pl.pallas_call(
        lambda *refs: select(table_count, *refs),
        out_shape=jax.ShapeDtypeStruct((table_count, batch, count), jnp.bfloat16),
        in_specs=[vmem] * 3,
        out_specs=vmem,
        compiler_params=small,
        cost_estimate=pl.CostEstimate(flops=40 * batch * count * table_count, bytes_accessed=4 * batch * count, transcendentals=0),
        name="select",
    )(jnp.stack(bags), jnp.stack(names), jnp.transpose(hot_ids, (1, 0, 2)))
    return pl.pallas_call(
        lambda *refs: pool(table_count, *refs),
        out_shape=jax.ShapeDtypeStruct((batch, table_count, width), jnp.float32),
        in_specs=[vmem] * 2,
        out_specs=vmem,
        compiler_params=small,
        name="pool",
    )(picks, second)


def solution(mesh):
    return jax.shard_map(
        body,
        mesh=mesh,
        in_specs=(
            P(None, AXES, None),
            P(AXES, None, None, None),
            P(AXES, None, None, None),
            P(),
            P(AXES, None, None),
        ),
        out_specs=P(AXES, None, None),
        check_vma=False,
    )
```

```python
import jax
import jax.numpy as jnp
from jax import lax
from jax.experimental import pallas as pl
from jax.experimental.pallas import tpu as pltpu
from jax.sharding import PartitionSpec as P


AXES = ("gx", "gy")


def push_hot(peers, depth, rows_dev, me_ref, order_ref, starts_ref, hot_ref, index_ref, table_ref, out_ref, sem):
    chunk = depth + 1
    listed = hot_ref.shape[1]
    out_ref[...] = jnp.zeros_like(out_ref)
    me = me_ref[0]
    start = starts_ref[me]
    count = starts_ref[me + 1] - start

    def one_entry(r, carry):
        place = start + r
        entry = order_ref[place]
        t = lax.div(entry, listed)
        row = hot_ref[t, entry - t * listed] - me * rows_dev
        pltpu.make_async_copy(
            table_ref.at[t * rows_dev + row],
            out_ref.at[lax.rem(place, peers) * chunk + lax.div(r, peers)],
            sem,
        ).start()
        return carry

    lax.fori_loop(0, count, one_entry, 0)
    for peer in range(peers):
        out_ref[peer * chunk + depth] = index_ref[peer]

    @pl.when(count > 0)
    def _():
        pltpu.make_async_copy(
            table_ref.at[pl.ds(0, count)], out_ref.at[pl.ds(0, count)], sem
        ).wait()


def look_up(peers, tables, slots, depth, hot, rows_dev, me_ref, starts_ref, rows_ref, hot_ref, table_ref, out_ref, hot_sc, sem):
    cold = tables * slots
    chunk = cold + hot

    def one_peer(peer, carry):
        for t in range(tables):
            for c in range(slots):
                row = rows_ref[peer, t * slots + c]
                pltpu.make_async_copy(
                    table_ref.at[t * rows_dev + row],
                    out_ref.at[peer * chunk + t * slots + c],
                    sem,
                ).start()
        return carry

    lax.fori_loop(0, peers, one_peer, 0)
    hot_sc[...] = jnp.zeros_like(hot_sc)
    me = me_ref[0]

    def one_owner(owner, carry):
        start = starts_ref[owner]
        count = starts_ref[owner + 1] - start
        first = lax.rem(me + hot * peers - start, peers)
        for d in range(depth):
            r = first + d * peers

            @pl.when(r < count)
            def _():
                hot_sc[lax.div(start + r, peers)] = hot_ref[owner, d]

        return carry

    lax.fori_loop(0, peers, one_owner, 0)
    total = hot_sc[...]
    for peer in range(peers):
        out_ref[pl.ds(peer * chunk + cold, hot)] = total
    pltpu.make_async_copy(
        table_ref.at[pl.ds(0, peers * cold)], out_ref.at[pl.ds(0, peers * cold)], sem
    ).wait()


def select(tables, bags_ref, names_ref, ids_ref, pick_ref):
    batch, count = pick_ref.shape[1:]
    sample = lax.broadcasted_iota(jnp.int32, (batch, count), 0)
    for t in range(tables):
        hits = (bags_ref[pl.ds(t, 1), :] == sample).astype(jnp.float32)
        names = names_ref[pl.ds(t, 1), :]
        for k in range(ids_ref.shape[2]):
            hits = hits + (ids_ref[t, :, k : k + 1] == names).astype(jnp.float32)
        pick_ref[t] = hits.astype(jnp.bfloat16)


def pool(tables, pick_ref, rows_ref, out_ref):
    rows = rows_ref[...]
    high = rows.astype(jnp.bfloat16)
    rest = rows - high.astype(jnp.float32)
    mid = rest.astype(jnp.bfloat16)
    low = (rest - mid.astype(jnp.float32)).astype(jnp.bfloat16)
    for t in range(tables):
        pick = pick_ref[t]
        part = jnp.dot(pick, low, preferred_element_type=jnp.float32)
        part = part + jnp.dot(pick, mid, preferred_element_type=jnp.float32)
        part = part + jnp.dot(pick, high, preferred_element_type=jnp.float32)
        out_ref[:, t, :] = part


def body(tables, cold_rows, cold_bags, hot_rows, hot_ids):
    peers = lax.axis_size("gx") * lax.axis_size("gy")
    table_count, rows_dev, width = tables.shape
    slots = cold_rows.shape[3]
    batch = hot_ids.shape[0]
    hot_count = hot_rows.shape[1]
    entries = table_count * hot_count
    hot = -(-entries // peers)
    cold = table_count * slots
    me = lax.axis_index(AXES).astype(jnp.int32).reshape(1)

    owner = lax.div(hot_rows.reshape(-1), jnp.int32(rows_dev))
    key = owner * entries + jnp.arange(entries, dtype=jnp.int32)
    rank = jnp.sum((key[None, :] < key[:, None]).astype(jnp.int32), axis=1)
    position = jnp.arange(hot * peers, dtype=jnp.int32)
    order = jnp.sum(jnp.where(rank[:, None] == position[None, :], jnp.arange(entries, dtype=jnp.int32)[:, None], 0), axis=0)
    order = jnp.where(position < entries, order, entries)
    starts = jnp.sum((owner[None, :] < jnp.arange(peers + 1, dtype=jnp.int32)[:, None]).astype(jnp.int32), axis=1)
    most = jnp.max(starts[1:] - starts[:-1])
    flat = tables.reshape(table_count * rows_dev, 1, width)
    lanes = -(-cold // width)
    assert lanes == 1
    wanted = jnp.transpose(cold_rows[0], (1, 0, 2)).reshape(peers, 1, cold).astype(jnp.float32)
    wanted = jnp.pad(wanted, ((0, 0), (0, 0), (0, width - cold)))

    smem = pl.BlockSpec(memory_space=pltpu.SMEM)
    vmem = pl.BlockSpec(memory_space=pltpu.VMEM)
    anywhere = pl.BlockSpec(memory_space=pl.ANY)
    small = pltpu.CompilerParams(vmem_limit_bytes=24 * 1024 * 1024)

    def gather(depth):
        first = pl.pallas_call(
            lambda *refs: push_hot(peers, depth, rows_dev, *refs),
            out_shape=jax.ShapeDtypeStruct((peers * (depth + 1), 1, width), jnp.float32),
            in_specs=[smem] * 4 + [vmem, anywhere],
            out_specs=vmem,
            scratch_shapes=[pltpu.SemaphoreType.DMA],
            name="push_hot",
        )(me, order, starts, hot_rows, wanted, flat)
        first = first.reshape(peers, depth + 1, 1, width)
        first = lax.all_to_all(first, AXES, split_axis=0, concat_axis=0, tiled=True)
        asked = first[:, depth, 0, :cold].astype(jnp.int32)
        return pl.pallas_call(
            lambda *refs: look_up(peers, table_count, slots, depth, hot, rows_dev, *refs),
            out_shape=jax.ShapeDtypeStruct((peers * (cold + hot), 1, width), jnp.float32),
            in_specs=[smem] * 3 + [vmem, anywhere],
            out_specs=vmem,
            scratch_shapes=[pltpu.VMEM((hot, 1, width), jnp.float32), pltpu.SemaphoreType.DMA],
            name="look_up",
        )(me, starts, asked, first, flat)

    narrow = min(2, hot)
    second = lax.cond(most <= narrow * peers, lambda: gather(narrow), lambda: gather(hot))
    second = second.reshape(peers, cold + hot, 1, width)
    second = lax.all_to_all(second, AXES, split_axis=0, concat_axis=0, tiled=True)
    second = second.reshape(peers * (cold + hot), width)

    bags = []
    names = []
    spread = jnp.transpose(order.reshape(hot, peers))
    for t in range(table_count):
        bags.append(jnp.pad(cold_bags[0, t], ((0, 0), (t * slots, cold + hot - (t + 1) * slots)), constant_values=-1).reshape(-1))
        name = spread - t * hot_count
        name = jnp.where(jnp.logical_and(name >= 0, name < hot_count), name, -1)
        names.append(jnp.pad(name, ((0, 0), (cold, 0)), constant_values=-1).reshape(-1))
    count = peers * (cold + hot)
    picks = pl.pallas_call(
        lambda *refs: select(table_count, *refs),
        out_shape=jax.ShapeDtypeStruct((table_count, batch, count), jnp.bfloat16),
        in_specs=[vmem] * 3,
        out_specs=vmem,
        compiler_params=small,
        cost_estimate=pl.CostEstimate(flops=40 * batch * count * table_count, bytes_accessed=4 * batch * count, transcendentals=0),
        name="select",
    )(jnp.stack(bags), jnp.stack(names), jnp.transpose(hot_ids, (1, 0, 2)))
    return pl.pallas_call(
        lambda *refs: pool(table_count, *refs),
        out_shape=jax.ShapeDtypeStruct((batch, table_count, width), jnp.float32),
        in_specs=[vmem] * 2,
        out_specs=vmem,
        compiler_params=small,
        name="pool",
    )(picks, second)


def solution(mesh):
    return jax.shard_map(
        body,
        mesh=mesh,
        in_specs=(
            P(None, AXES, None),
            P(AXES, None, None, None),
            P(AXES, None, None, None),
            P(),
            P(AXES, None, None),
        ),
        out_specs=P(AXES, None, None),
        check_vma=False,
    )
```

```python
import jax
import jax.numpy as jnp
from jax import lax
from jax.experimental import pallas as pl
from jax.experimental.pallas import tpu as pltpu
from jax.sharding import PartitionSpec as P


AXES = ("gx", "gy")


def push_hot(peers, depth, rows_dev, me_ref, order_ref, starts_ref, hot_ref, index_ref, table_ref, out_ref, sem):
    chunk = depth + 1
    listed = hot_ref.shape[1]
    out_ref[...] = jnp.zeros_like(out_ref)
    me = me_ref[0]
    start = starts_ref[me]
    count = starts_ref[me + 1] - start

    def one_entry(r, carry):
        place = start + r
        entry = order_ref[place]
        t = lax.div(entry, listed)
        row = hot_ref[t, entry - t * listed] - me * rows_dev
        pltpu.make_async_copy(
            table_ref.at[t * rows_dev + row],
            out_ref.at[lax.rem(place, peers) * chunk + lax.div(r, peers)],
            sem,
        ).start()
        return carry

    lax.fori_loop(0, count, one_entry, 0)
    for peer in range(peers):
        out_ref[peer * chunk + depth] = index_ref[peer]

    @pl.when(count > 0)
    def _():
        pltpu.make_async_copy(
            table_ref.at[pl.ds(0, count)], out_ref.at[pl.ds(0, count)], sem
        ).wait()


def look_up(peers, tables, slots, depth, hot, rows_dev, me_ref, starts_ref, rows_ref, hot_ref, table_ref, out_ref, hot_sc, sem):
    cold = tables * slots
    chunk = cold + hot

    def one_peer(peer, carry):
        for t in range(tables):
            for c in range(slots):
                row = rows_ref[peer, t * slots + c]
                pltpu.make_async_copy(
                    table_ref.at[t * rows_dev + row],
                    out_ref.at[peer * chunk + t * slots + c],
                    sem,
                ).start(priority=c % 2)
        return carry

    lax.fori_loop(0, peers, one_peer, 0)
    hot_sc[...] = jnp.zeros_like(hot_sc)
    me = me_ref[0]

    def one_owner(owner, carry):
        start = starts_ref[owner]
        count = starts_ref[owner + 1] - start
        first = lax.rem(me + hot * peers - start, peers)
        for d in range(depth):
            r = first + d * peers

            @pl.when(r < count)
            def _():
                hot_sc[lax.div(start + r, peers)] = hot_ref[owner, d]

        return carry

    lax.fori_loop(0, peers, one_owner, 0)
    total = hot_sc[...]
    for peer in range(peers):
        out_ref[pl.ds(peer * chunk + cold, hot)] = total
    pltpu.make_async_copy(
        table_ref.at[pl.ds(0, peers * cold)], out_ref.at[pl.ds(0, peers * cold)], sem
    ).wait()


def select(tables, bags_ref, names_ref, ids_ref, pick_ref):
    batch, count = pick_ref.shape[1:]
    sample = lax.broadcasted_iota(jnp.int32, (batch, count), 0)
    for t in range(tables):
        hits = (bags_ref[pl.ds(t, 1), :] == sample).astype(jnp.float32)
        names = names_ref[pl.ds(t, 1), :]
        for k in range(ids_ref.shape[2]):
            hits = hits + (ids_ref[t, :, k : k + 1] == names).astype(jnp.float32)
        pick_ref[t] = hits.astype(jnp.bfloat16)


def pool(tables, pick_ref, rows_ref, out_ref):
    rows = rows_ref[...]
    high = rows.astype(jnp.bfloat16)
    rest = rows - high.astype(jnp.float32)
    mid = rest.astype(jnp.bfloat16)
    low = (rest - mid.astype(jnp.float32)).astype(jnp.bfloat16)
    for t in range(tables):
        pick = pick_ref[t]
        part = jnp.dot(pick, low, preferred_element_type=jnp.float32)
        part = part + jnp.dot(pick, mid, preferred_element_type=jnp.float32)
        part = part + jnp.dot(pick, high, preferred_element_type=jnp.float32)
        out_ref[:, t, :] = part


def body(tables, cold_rows, cold_bags, hot_rows, hot_ids):
    peers = lax.axis_size("gx") * lax.axis_size("gy")
    table_count, rows_dev, width = tables.shape
    slots = cold_rows.shape[3]
    batch = hot_ids.shape[0]
    hot_count = hot_rows.shape[1]
    entries = table_count * hot_count
    hot = -(-entries // peers)
    cold = table_count * slots
    me = lax.axis_index(AXES).astype(jnp.int32).reshape(1)

    owner = lax.div(hot_rows.reshape(-1), jnp.int32(rows_dev))
    key = owner * entries + jnp.arange(entries, dtype=jnp.int32)
    rank = jnp.sum((key[None, :] < key[:, None]).astype(jnp.int32), axis=1)
    position = jnp.arange(hot * peers, dtype=jnp.int32)
    order = jnp.sum(jnp.where(rank[:, None] == position[None, :], jnp.arange(entries, dtype=jnp.int32)[:, None], 0), axis=0)
    order = jnp.where(position < entries, order, entries)
    starts = jnp.sum((owner[None, :] < jnp.arange(peers + 1, dtype=jnp.int32)[:, None]).astype(jnp.int32), axis=1)
    most = jnp.max(starts[1:] - starts[:-1])
    flat = tables.reshape(table_count * rows_dev, 1, width)
    lanes = -(-cold // width)
    assert lanes == 1
    wanted = jnp.transpose(cold_rows[0], (1, 0, 2)).reshape(peers, 1, cold).astype(jnp.float32)
    wanted = jnp.pad(wanted, ((0, 0), (0, 0), (0, width - cold)))

    smem = pl.BlockSpec(memory_space=pltpu.SMEM)
    vmem = pl.BlockSpec(memory_space=pltpu.VMEM)
    anywhere = pl.BlockSpec(memory_space=pl.ANY)
    small = pltpu.CompilerParams(vmem_limit_bytes=24 * 1024 * 1024)

    def gather(depth):
        first = pl.pallas_call(
            lambda *refs: push_hot(peers, depth, rows_dev, *refs),
            out_shape=jax.ShapeDtypeStruct((peers * (depth + 1), 1, width), jnp.float32),
            in_specs=[smem] * 4 + [vmem, anywhere],
            out_specs=vmem,
            scratch_shapes=[pltpu.SemaphoreType.DMA],
            name="push_hot",
        )(me, order, starts, hot_rows, wanted, flat)
        first = first.reshape(peers, depth + 1, 1, width)
        first = lax.all_to_all(first, AXES, split_axis=0, concat_axis=0, tiled=True)
        asked = first[:, depth, 0, :cold].astype(jnp.int32)
        return pl.pallas_call(
            lambda *refs: look_up(peers, table_count, slots, depth, hot, rows_dev, *refs),
            out_shape=jax.ShapeDtypeStruct((peers * (cold + hot), 1, width), jnp.float32),
            in_specs=[smem] * 3 + [vmem, anywhere],
            out_specs=vmem,
            scratch_shapes=[pltpu.VMEM((hot, 1, width), jnp.float32), pltpu.SemaphoreType.DMA],
            name="look_up",
        )(me, starts, asked, first, flat)

    narrow = min(2, hot)
    second = lax.cond(most <= narrow * peers, lambda: gather(narrow), lambda: gather(hot))
    second = second.reshape(peers, cold + hot, 1, width)
    second = lax.all_to_all(second, AXES, split_axis=0, concat_axis=0, tiled=True)
    second = second.reshape(peers * (cold + hot), width)

    bags = []
    names = []
    spread = jnp.transpose(order.reshape(hot, peers))
    for t in range(table_count):
        bags.append(jnp.pad(cold_bags[0, t], ((0, 0), (t * slots, cold + hot - (t + 1) * slots)), constant_values=-1).reshape(-1))
        name = spread - t * hot_count
        name = jnp.where(jnp.logical_and(name >= 0, name < hot_count), name, -1)
        names.append(jnp.pad(name, ((0, 0), (cold, 0)), constant_values=-1).reshape(-1))
    count = peers * (cold + hot)
    picks = pl.pallas_call(
        lambda *refs: select(table_count, *refs),
        out_shape=jax.ShapeDtypeStruct((table_count, batch, count), jnp.bfloat16),
        in_specs=[vmem] * 3,
        out_specs=vmem,
        compiler_params=small,
        cost_estimate=pl.CostEstimate(flops=40 * batch * count * table_count, bytes_accessed=4 * batch * count, transcendentals=0),
        name="select",
    )(jnp.stack(bags), jnp.stack(names), jnp.transpose(hot_ids, (1, 0, 2)))
    return pl.pallas_call(
        lambda *refs: pool(table_count, *refs),
        out_shape=jax.ShapeDtypeStruct((batch, table_count, width), jnp.float32),
        in_specs=[vmem] * 2,
        out_specs=vmem,
        compiler_params=small,
        name="pool",
    )(picks, second)


def solution(mesh):
    return jax.shard_map(
        body,
        mesh=mesh,
        in_specs=(
            P(None, AXES, None),
            P(AXES, None, None, None),
            P(AXES, None, None, None),
            P(),
            P(AXES, None, None),
        ),
        out_specs=P(AXES, None, None),
        check_vma=False,
    )
```
